32 devices in a mesh: blk: 8 (over z, y), layer: 4 (over x, core).
Axes of the slice: x: 2, y: 2, z: 4, core: 2. Of those that a mesh axis runs over, the one named last changes fastest.
Arguments:
- leaf_area: float32 [12, 16, 1024], P(None, 'layer', 'blk'), may hold values from 0 to 6
- soil_water: float32 [10, 1024], P(None, 'blk'), may hold values from 0.05 to 0.5
- root_share: float32 [16, 10], P('layer'), may hold values from 0 to 0.3
- patch_weight: float32 [16, 32768], P('layer', 'blk'), may hold values from 0 to 1
- patch_owner: int32 [32768, 1], P('blk'), may hold values from 0 to 7; in each aligned block of 4096 rows (0 to 4095, 4096 to 8191, ...) at most 1024 rows name the same one
- patch_local: int32 [32768], P('blk'), may hold values from 0 to 127
- month: int32 [1], replicated, may hold values from 0 to 11
- mix: float32 [1], replicated, may hold values from 0.1 to 0.9
Outputs:
- canopy_share: float32 [16, 1024], P('layer', 'blk')
The draws below stay inside these ranges and needn't reach their ends.
Inputs may be any that keep to these rules, and one draw needn't show every extreme that they name: `patch_owner`: among the rows of one device, no owner is named more than 1024 times, a bound that some block reaches.
All inputs are finite; a program needn't handle non-finite values.
Results may differ from the reference program's by a relative error of at most 0.000065.
Values sent between devices are 32-bit elements; how exact they have to be, the bound alone decides.
A program may use at most 64 MiB of HBM per device.

```python
import math
import jax
import jax.numpy as jnp
import numpy as np
from jax import lax

PFT = 16
MONTHS = 12
SOIL = 10
G_DEV = 128
P_DEV = 4096
GRID = 1024
PATCHES = 32768
CAP = 1024
N_BLK = 8


def touch_ends(drawn, rng, low, top_value):
    spot = [jax.random.randint(jax.random.fold_in(rng, axis), (), 0, length) for axis, length in enumerate(drawn.shape)]
    longest = drawn.shape.index(max(drawn.shape))
    next_to = spot[:longest] + [(spot[longest] + 1) % drawn.shape[longest]] + spot[longest + 1:]
    return drawn.at[tuple(spot)].set(low).at[tuple(next_to)].set(top_value)


def level_of(own_key, extent, pieces, low, top_value):
    def one(axis_at, parts):
        steps = jax.random.uniform(jax.random.fold_in(jax.random.fold_in(own_key, 6), axis_at), (parts,), jnp.float32, low / len(pieces), top_value / len(pieces))
        return jnp.repeat(jnp.exp(steps), extent[axis_at] // parts).reshape((-1,) + (1,) * (len(extent) - axis_at - 1))

    gain = one(*pieces[0])
    for cut in pieces[1:]:
        gain = gain * one(*cut)
    return gain


def assign_block(stream_key, own, number, rows, count, top, most, skew):
    ranking = jax.random.permutation(stream_key, count)
    heavy_load, usual = load_shares(count, rows * top, most, skew, True), load_shares(count, rows * top, most, skew, False)
    places = jnp.arange(count)

    def named(lengths, rotation):
        used = int((lengths > 0).sum())
        fixed = max(1, used // 4)
        passed = fixed + (places - fixed + rotation * (used - fixed)) % max(1, count - fixed)
        return jnp.zeros((count,), jnp.int32).at[ranking[jnp.where(places < fixed, places, passed)]].set(jnp.asarray(lengths, jnp.int32))

    lengths = jnp.where(number % 4 == 0, named(heavy_load, number // 4), named(usual, number - number // 4 - 1))
    mixed = jax.random.permutation(jax.random.fold_in(own, 3), count)
    source_of, receiver = mixed[0:count // 2 * 2:2], mixed[1:count // 2 * 2:2]
    margin = jnp.minimum(lengths[source_of] - 1, most - lengths[receiver]) // 2
    margin = jnp.where((source_of == ranking[0]) | (receiver == ranking[0]) | (lengths[receiver] == 0), 0, jnp.maximum(margin, 0))
    passed = jax.random.randint(jax.random.fold_in(own, 4), (count // 2,), 0, 1 << 20) % (margin + 1)
    lengths = lengths.at[source_of].add(-passed).at[receiver].add(passed)
    items = jnp.searchsorted(jnp.cumsum(lengths), jnp.arange(rows * top), side="right").astype(jnp.int32)
    table = items.reshape(top, rows).T
    table = table[jax.random.permutation(jax.random.fold_in(own, 1), rows)]
    rotation = jax.random.randint(jax.random.fold_in(own, 2), (rows, 1), 0, top)
    return jnp.take_along_axis(table, (jnp.arange(top)[None, :] + rotation) % top, axis=1)


def load_shares(count, total, reach, skew, full):
    weights = [(1 << 20) // math.isqrt(standing ** skew) + 1 for standing in range(1, count + 1)]
    largest = reach if full else min(reach, max(-(-total // count), total * weights[0] // sum(weights)))
    least = 1 if total - largest >= count - 1 else 0
    counts, surplus = [largest] + [least] * (count - 1), total - largest - least * (count - 1)
    while surplus > 0:
        free = [i for i in range(1, count) if counts[i] < largest] or [i for i in range(1, count) if counts[i] < reach]
        mass, left = sum([weights[i] for i in free]), surplus
        for i in free:
            addition = min(reach - counts[i], max(1, left * weights[i] // mass), surplus)
            counts[i] = counts[i] + addition
            surplus = surplus - addition
    return np.array(counts)


def setup_inputs(seed: int = 0) -> dict:
    keys = jax.random.split(jax.random.key(seed), 9)
    leaf_area = jnp.clip(6.0 * jax.random.uniform(keys[0], (MONTHS, PFT, GRID), jnp.float32) ** level_of(keys[0], (MONTHS, PFT, GRID), ((1, 4), (2, 8)), -0.2, 0.2), 0.0, 6.0)
    soil_water = jnp.clip(0.05 + 0.45 * jax.random.uniform(keys[1], (SOIL, GRID), jnp.float32) ** level_of(keys[1], (SOIL, GRID), ((1, 8),), -0.2, 0.2), 0.05, 0.5)
    root_share = jnp.clip(0.3 * jax.random.uniform(keys[2], (PFT, SOIL), jnp.float32) ** level_of(keys[2], (PFT, SOIL), ((0, 4),), -0.2, 0.2), 0.0, 0.3)
    patch_weight = jnp.clip(1.0 * jax.random.uniform(keys[3], (PFT, PATCHES), jnp.float32) ** level_of(keys[3], (PFT, PATCHES), ((0, 4), (1, 8)), -0.2, 0.2), 0.0, 1.0)
    patch_owner_keys = jax.random.split(jax.random.fold_in(keys[4], 1), PATCHES // P_DEV)
    patch_owner_turns = jax.random.permutation(jax.random.fold_in(keys[4], 3), PATCHES // P_DEV)
    patch_owner = jax.vmap(lambda own, number: assign_block(jax.random.fold_in(keys[4], 2), own, number, P_DEV, N_BLK, 1, CAP, 2))(patch_owner_keys, patch_owner_turns).reshape((PATCHES, 1))
    patch_local = touch_ends(jax.random.randint(keys[5], (PATCHES,), 0, G_DEV), jax.random.fold_in(keys[5], 1), 0, G_DEV - 1).astype(jnp.int32)
    month = jax.random.randint(keys[6], (1,), 0, MONTHS).astype(jnp.int32)
    mix = jnp.clip(jax.random.uniform(keys[7], (1,), jnp.float32, 0.1, 0.9), 0.1, 0.9)
    return dict(leaf_area=leaf_area, soil_water=soil_water, root_share=root_share, patch_weight=patch_weight, patch_owner=patch_owner, patch_local=patch_local, month=month, mix=mix)


def interpolate(leaf_area, month, mix):
    earlier_index = month[0]
    second = (earlier_index + 1) % MONTHS
    earlier = lax.dynamic_index_in_dim(leaf_area, earlier_index, 0, keepdims=False)
    later = lax.dynamic_index_in_dim(leaf_area, second, 0, keepdims=False)
    return mix[0] * earlier + (1.0 - mix[0]) * later


def reference(leaf_area, soil_water, root_share, patch_weight, patch_owner, patch_local, month, mix):
    patch_cell = (patch_owner[:, 0] * G_DEV + patch_local).astype(jnp.int32)
    current = interpolate(leaf_area, month, mix)
    patch_leaf = jnp.take(current, patch_cell, axis=1)
    patch_soil = jnp.take(soil_water, patch_cell, axis=1)
    stress = jnp.dot(root_share, patch_soil, precision=lax.Precision.HIGHEST)
    canopy = patch_weight * (1.0 - jnp.exp(-0.5 * patch_leaf)) * stress
    grid_sum = jax.ops.segment_sum(canopy.T, patch_cell, num_segments=GRID).T
    total = jnp.sum(grid_sum, axis=0)
    return grid_sum / (1.0 + total)
```

```python
import functools

import jax
import jax.numpy as jnp
from jax import lax
from jax.experimental import pallas as pl
from jax.experimental.pallas import tpu as pltpu
from jax.sharding import PartitionSpec as P

MESH = pl.DeviceIdType.MESH
CHUNK = 512


def local_sums(weight, owner, local, owners, cells):
    types, patches = weight.shape
    chunk = CHUNK if patches % CHUNK == 0 else patches
    row_owner = lax.broadcasted_iota(jnp.int32, (owners * types, chunk), 0) // types
    cell = lax.broadcasted_iota(jnp.int32, (cells, chunk), 0)
    total = None
    for start in range(0, patches, chunk):
        part = slice(start, start + chunk)
        w = weight[:, part]
        high = w.astype(jnp.bfloat16).astype(jnp.float32)
        low = w - high
        named = row_owner == owner[:, part]
        left = jnp.concatenate(
            [
                jnp.where(named, jnp.concatenate([piece] * owners, axis=0), 0.0)
                for piece in (high, low)
            ],
            axis=0,
        ).astype(jnp.bfloat16)
        table = jnp.where(cell == local[:, part], 1.0, 0.0).astype(jnp.bfloat16)
        product = lax.dot_general(
            left, table, (((1,), (1,)), ((), ())), preferred_element_type=jnp.float32
        )
        total = product if total is None else total + product
    return total[: owners * types] + total[owners * types :]


def month_weights(month, mix, out):
    row = lax.broadcasted_iota(jnp.int32, out.shape, 0)
    first = month[0]
    second = lax.rem(first + 1, out.shape[0])
    blend = jnp.where(row == second, 1.0 - mix[0], 0.0)
    out[...] = jnp.where(row == first, mix[0], blend)


def blank(out):
    out[...] = jnp.zeros(out.shape, out.dtype)


def exchange(
    n, m, blend, leaf_hbm, soil_hbm, root_hbm, weight_hbm, owner_hbm, local_hbm,
    sums_out, leaf_out, stress_out, soil, root, weight, owner, local,
    sums, got_sums, load_sem, send_sem, recv_sem,
):
    blk, layer = lax.axis_index("blk"), lax.axis_index("layer")
    types, cells = sums_out.shape[1:]
    loads = [
        pltpu.make_async_copy(source, target, load_sem.at[i])
        for i, (source, target) in enumerate(
            (
                (weight_hbm, weight),
                (owner_hbm, owner),
                (local_hbm, local),
                (leaf_hbm, leaf_out.at[0]),
                (soil_hbm, soil),
                (root_hbm, root),
            )
        )
    ]
    for load in loads:
        load.start()

    def device(step_blk, step_layer):
        return (lax.rem(blk + step_blk, n), lax.rem(layer + step_layer, m))

    steps = [(i, j) for i in range(n) for j in range(m) if i or j]
    barrier = pltpu.get_barrier_semaphore()
    for step in steps:
        pl.semaphore_signal(barrier, inc=1, device_id=device(*step), device_id_type=MESH)

    for load in loads[:3]:
        load.wait()
    partial = local_sums(weight, owner, local, n, cells)
    for i in range(n):
        sums[i] = partial[i * types : (i + 1) * types]
    for load in loads[3:]:
        load.wait()
    stress = root[:, 0:1] * soil[0:1, :]
    for i in range(1, soil.shape[0]):
        stress += root[:, i : i + 1] * soil[i : i + 1, :]
    stress_out[0] = stress
    own = sums[blk]

    pl.semaphore_wait(barrier, len(steps))

    def send(source, target, k, i, j):
        pltpu.make_async_remote_copy(
            src_ref=source,
            dst_ref=target,
            send_sem=send_sem.at[k],
            recv_sem=recv_sem.at[k],
            device_id=device(i, j),
            device_id_type=MESH,
        ).start()

    for i, j in steps:
        if i:
            send(sums.at[lax.rem(blk + i, n)], got_sums.at[j * (n - 1) + i - 1], 0, i, j)
        else:
            send(sums.at[blk], got_sums.at[m * (n - 1) + j - 1], 0, i, j)
    for j in range(1, m):
        send(stress_out.at[0], stress_out.at[j], 1, 0, j)
        send(leaf_out.at[0], leaf_out.at[j], 2, 0, j)
    pltpu.make_async_copy(got_sums, got_sums, recv_sem.at[0]).wait()
    for j in range(m):
        grid = own if j == 0 else got_sums[m * (n - 1) + j - 1]
        for i in range(n - 1):
            grid = grid + got_sums[j * (n - 1) + i]
        sums_out[j] = grid
    rest = stress_out.at[pl.ds(1, m - 1)], leaf_out.at[pl.ds(1, m - 1)]
    for k, ref in enumerate(rest):
        pltpu.make_async_copy(ref, ref, recv_sem.at[k + 1]).wait()
    pltpu.make_async_copy(got_sums, got_sums, send_sem.at[0]).wait()
    for k, ref in enumerate(rest):
        pltpu.make_async_copy(ref, ref, send_sem.at[k + 1]).wait()


def share(current, sums, stress):
    grid = sums[...] * (1.0 - jnp.exp(-0.5 * current)) * stress[...]
    return grid[0] / (1.0 + jnp.sum(grid, axis=(0, 1), keepdims=True)[0])


def finish_blend(sums, leaf, stress, blend, out):
    current = blend[0] * leaf[:, 0]
    for k in range(1, leaf.shape[1]):
        current += blend[k] * leaf[:, k]
    out[...] = share(current, sums, stress)


def finish_scalars(sums, leaf, stress, month, mix, out):
    first = month[0]
    second = lax.rem(first + 1, leaf.shape[1])
    current = mix[0] * leaf[:, first] + (1.0 - mix[0]) * leaf[:, second]
    out[...] = share(current, sums, stress)


def on_device(
    leaf_area, soil_water, root_share, patch_weight, patch_owner, patch_local, month, mix
):
    n, m = lax.axis_size("blk"), lax.axis_size("layer")
    months, types, cells = leaf_area.shape
    patches = patch_local.shape[0]
    owner = patch_owner.reshape(1, patches)
    local = patch_local.reshape(1, patches)
    f32, i32 = jnp.float32, jnp.int32
    hbm = pl.BlockSpec(memory_space=pl.ANY)
    vmem = pl.BlockSpec(memory_space=pltpu.VMEM)
    smem = pl.BlockSpec(memory_space=pltpu.SMEM)
    early = lax.axis_index("blk") * m + lax.axis_index("layer") < 2
    blend_shape = jax.ShapeDtypeStruct((months, 1, cells), f32)

    def weigh(month, mix):
        return pl.pallas_call(month_weights, out_shape=blend_shape, in_specs=[smem] * 2, out_specs=vmem)(month, mix)

    def skip(month, mix):
        return pl.pallas_call(blank, out_shape=blend_shape, out_specs=vmem)()

    blend = lax.cond(early, weigh, skip, month, mix)

    sums, leaf, stress = pl.pallas_call(
        functools.partial(exchange, n, m),
        out_shape=[
            pltpu.VMEM((m, types, cells), f32),
            pltpu.VMEM((m, months, types, cells), f32),
            pltpu.VMEM((m, types, cells), f32),
        ],
        in_specs=[vmem] + [hbm] * 6,
        out_specs=[vmem] * 3,
        scratch_shapes=[
            pltpu.VMEM(soil_water.shape, f32),
            pltpu.VMEM(root_share.shape, f32),
            pltpu.VMEM(patch_weight.shape, f32),
            pltpu.VMEM(owner.shape, i32),
            pltpu.VMEM(local.shape, i32),
            pltpu.VMEM((n, types, cells), f32),
            pltpu.VMEM((m * (n - 1) + m - 1, types, cells), f32),
            pltpu.SemaphoreType.DMA((6,)),
            pltpu.SemaphoreType.DMA((3,)),
            pltpu.SemaphoreType.DMA((3,)),
        ],
        compiler_params=pltpu.CompilerParams(collective_id=0, has_side_effects=True),
    )(blend, leaf_area, soil_water, root_share, patch_weight, owner, local)

    out_shape = jax.ShapeDtypeStruct((types, cells), f32)

    def early_finish(sums, leaf, stress, blend, month, mix):
        return pl.pallas_call(finish_blend, out_shape=out_shape, in_specs=[vmem] * 4, out_specs=vmem)(sums, leaf, stress, blend)

    def late_finish(sums, leaf, stress, blend, month, mix):
        return pl.pallas_call(finish_scalars, out_shape=out_shape, in_specs=[vmem] * 3 + [smem] * 2, out_specs=vmem)(sums, leaf, stress, month, mix)

    return lax.cond(early, early_finish, late_finish, sums, leaf, stress, blend, month, mix)


def solution(mesh):
    in_specs = (
        P(None, "layer", "blk"),
        P(None, "blk"),
        P("layer", None),
        P("layer", "blk"),
        P("blk", None),
        P("blk"),
        P(),
        P(),
    )
    out_specs = P("layer", "blk")
    return jax.shard_map(
        on_device, mesh=mesh, in_specs=in_specs, out_specs=out_specs, check_vma=False
    )
```

```python
import functools

import jax
import jax.numpy as jnp
from jax import lax
from jax.experimental import pallas as pl
from jax.experimental.pallas import tpu as pltpu
from jax.sharding import PartitionSpec as P

MESH = pl.DeviceIdType.MESH
CHUNK = 512
NEAR = 2


def local_sums(weight, owner, local, owners, cells):
    types, patches = weight.shape
    chunk = CHUNK if patches % CHUNK == 0 else patches
    tall = 16
    rows = lax.broadcasted_iota(jnp.int32, (tall, chunk), 0) // types
    groups = owners * types // tall
    per = tall // types
    row_owner = [(rows + per * g).astype(jnp.int16) for g in range(groups)]
    cell = lax.broadcasted_iota(jnp.int32, (cells, chunk), 0).astype(jnp.int16)
    zero, one = jnp.bfloat16(0.0), jnp.bfloat16(1.0)
    total = None
    for start in range(0, patches, chunk):
        part = slice(start, start + chunk)
        w = weight[:, part]
        w = jnp.concatenate([w] * (8 // types), axis=0)
        high = w.astype(jnp.bfloat16).astype(jnp.float32)
        low = w - high
        high, low = [
            jnp.concatenate([piece] * (tall // 8), axis=0).astype(jnp.bfloat16)
            for piece in (high, low)
        ]
        who = jnp.broadcast_to(owner[:, part], (tall, chunk)).astype(jnp.int16)
        named = [row == who for row in row_owner]
        left = jnp.concatenate(
            [jnp.where(name, piece, zero) for piece in (high, low) for name in named], axis=0
        )
        where = jnp.broadcast_to(local[:, part], (tall, chunk)).astype(jnp.int16)
        where = jnp.concatenate([where] * (cells // tall), axis=0)
        table = jnp.where(cell == where, one, zero).astype(jnp.float8_e4m3fn)
        product = lax.dot_general(
            left, table, (((1,), (1,)), ((), ())), preferred_element_type=jnp.float32
        )
        total = product if total is None else total + product
    return total[: owners * types] + total[owners * types :]


def spread(value, out):
    out[...] = jnp.zeros(out.shape, out.dtype) + value[0].astype(out.dtype)


def blank(out):
    out[...] = jnp.zeros(out.shape, out.dtype)


def kernel(
    n, m, given, leaf_hbm, soil_hbm, root_hbm, weight_hbm, owner_hbm, local_hbm,
    out_ref, soil, root, weight, owner, local, leaf, scalars, sums, pairs, got,
    load_sem, send_sem, recv_sem, met_sem,
):
    blk, layer = lax.axis_index("blk"), lax.axis_index("layer")
    types, cells = out_ref.shape
    months = leaf.shape[1]
    everywhere = [(b, k) for b in range(n) for k in range(m)]
    is_near = jnp.logical_and(blk == 0, layer >= NEAR)
    pair_sem, leaf_sem, scalar_sem = n, n + 1, n + 2
    loads = [
        pltpu.make_async_copy(source, target, load_sem.at[i])
        for i, (source, target) in enumerate(
            (
                (weight_hbm, weight),
                (owner_hbm, owner),
                (local_hbm, local),
                (soil_hbm, soil),
                (root_hbm, root),
                (leaf_hbm, leaf.at[layer]),
            )
        )
    ]
    for load in loads:
        load.start()

    barrier = pltpu.get_barrier_semaphore()

    def greet(semaphore, b, k):
        pl.semaphore_signal(semaphore, inc=1, device_id=(b, k), device_id_type=MESH)

    peers = [lax.rem(layer + j, m) for j in range(1, m)]
    for k in peers:
        greet(barrier, blk, k)
    for b in range(n):

        @pl.when(blk != b)
        def _():
            for k in range(m if b else min(NEAR, m)):
                greet(barrier, b, k)

    for load in loads[:3]:
        load.wait()
    partial = local_sums(weight, owner, local, n, cells)
    for i in range(n):
        sums[i] = partial[i * types : (i + 1) * types]
    for load in loads[3:]:
        load.wait()
    stress = root[:, 0:1] * soil[0:1, :]
    for i in range(1, soil.shape[0]):
        stress += root[:, i : i + 1] * soil[i : i + 1, :]
    pairs[layer, 0] = sums[blk]
    pairs[layer, 1] = stress
    got[blk] = jnp.zeros(got.shape[1:], got.dtype)

    def send(source, target, sem, b, k):
        pltpu.make_async_remote_copy(
            src_ref=source,
            dst_ref=target,
            send_sem=send_sem.at[sem],
            recv_sem=recv_sem.at[sem],
            device_id=(b, k),
            device_id_type=MESH,
        ).start()

    def send_peers():
        for k in peers:
            send(pairs.at[layer], pairs.at[layer], pair_sem, blk, k)
        for k in peers:
            send(leaf.at[layer], leaf.at[layer], leaf_sem, blk, k)

    pl.semaphore_wait(barrier, jnp.where(is_near, m - 1, n * m - 1))

    @pl.when(is_near)
    def _():
        send_peers()
        pl.semaphore_wait(met_sem, (n - 1) * m)

    for b in range(n):

        @pl.when(blk != b)
        def _():
            for k in range(m):
                send(sums.at[b], got.at[blk, layer], blk, b, k)
            if b == 0:
                for k in range(NEAR, m):
                    greet(met_sem, 0, k)

    pl.when(jnp.logical_not(is_near))(send_peers)

    reads = [jnp.logical_and(blk == 0, layer == k) for k in range(2)]
    for k, read in enumerate(reads):
        row = scalars.at[k]

        @pl.when(read)
        def _():
            for place in everywhere:
                if place != (0, k):
                    send(given, row, scalar_sem + k, *place)
            row[...] = given[...]

        @pl.when(jnp.logical_not(read))
        def _():
            pltpu.make_async_copy(row, row, recv_sem.at[scalar_sem + k]).wait()

    others = pl.ds(0, m - 1)
    arrivals = [(pairs.at[others], pair_sem), (leaf.at[others], leaf_sem)]
    for ref, sem in arrivals:
        pltpu.make_async_copy(ref, ref, recv_sem.at[sem]).wait()
    first, mix = scalars[0], scalars[1]
    second = jnp.where(first == months - 1, 0.0, first + 1.0)
    share = [
        jnp.where(first == k, mix, jnp.where(second == k, 1.0 - mix, 0.0)) for k in range(months)
    ]
    effects, grids = [], []
    for k in range(m):
        current = share[0] * leaf[k, 0]
        for i in range(1, months):
            current += share[i] * leaf[k, i]
        effects.append((1.0 - jnp.exp(-0.5 * current)) * pairs[k, 1])
        grids.append(pairs[k, 0])
    for b in range(n):

        @pl.when(blk != b)
        def _():
            pltpu.make_async_copy(got.at[b], got.at[b], recv_sem.at[b]).wait()

        grids = [grid + got[b, k] for k, grid in enumerate(grids)]
    mine, everyone = None, None
    for k in range(m):
        grid = grids[k] * effects[k]
        mine = grid if k == 0 else jnp.where(layer == k, grid, mine)
        everyone = grid if k == 0 else everyone + grid
    out_ref[...] = mine / (1.0 + jnp.sum(everyone, axis=0, keepdims=True))

    sent = got.at[pl.ds(0, n - 1)]
    pltpu.make_async_copy(sent, sent, send_sem.at[blk]).wait()
    for ref, sem in arrivals:
        pltpu.make_async_copy(ref, ref, send_sem.at[sem]).wait()
    for k, read in enumerate(reads):
        row = scalars.at[k]

        @pl.when(read)
        def _():
            for _ in everywhere[1:]:
                pltpu.make_async_copy(row, row, send_sem.at[scalar_sem + k]).wait()


def on_device(
    leaf_area, soil_water, root_share, patch_weight, patch_owner, patch_local, month, mix
):
    n, m = lax.axis_size("blk"), lax.axis_size("layer")
    months, types, cells = leaf_area.shape
    patches = patch_local.shape[0]
    owner = patch_owner.reshape(1, patches)
    local = patch_local.reshape(1, patches)
    f32, i32 = jnp.float32, jnp.int32
    hbm = pl.BlockSpec(memory_space=pl.ANY)
    vmem = pl.BlockSpec(memory_space=pltpu.VMEM)
    smem = pl.BlockSpec(memory_space=pltpu.SMEM)
    row = jax.ShapeDtypeStruct((1, cells), f32)

    def reader(value):
        return pl.pallas_call(spread, out_shape=row, in_specs=[smem], out_specs=vmem)(value)

    role = jnp.where(lax.axis_index("blk") == 0, jnp.minimum(lax.axis_index("layer"), 2), 2)
    given = lax.switch(
        role,
        [
            lambda month, mix: reader(month),
            lambda month, mix: reader(mix),
            lambda month, mix: pl.pallas_call(blank, out_shape=row, out_specs=vmem)(),
        ],
        month,
        mix,
    )
    return pl.pallas_call(
        functools.partial(kernel, n, m),
        out_shape=pltpu.VMEM((types, cells), f32),
        in_specs=[vmem] + [hbm] * 6,
        out_specs=vmem,
        scratch_shapes=[
            pltpu.VMEM(soil_water.shape, f32),
            pltpu.VMEM(root_share.shape, f32),
            pltpu.VMEM(patch_weight.shape, f32),
            pltpu.VMEM(owner.shape, i32),
            pltpu.VMEM(local.shape, i32),
            pltpu.VMEM((m, months, types, cells), f32),
            pltpu.VMEM((2, *row.shape), f32),
            pltpu.VMEM((n, types, cells), f32),
            pltpu.VMEM((m, 2, types, cells), f32),
            pltpu.VMEM((n, m, types, cells), f32),
            pltpu.SemaphoreType.DMA((6,)),
            pltpu.SemaphoreType.DMA((n + 4,)),
            pltpu.SemaphoreType.DMA((n + 4,)),
            pltpu.SemaphoreType.REGULAR,
        ],
        compiler_params=pltpu.CompilerParams(collective_id=0, has_side_effects=True),
    )(given, leaf_area, soil_water, root_share, patch_weight, owner, local)


def solution(mesh):
    in_specs = (
        P(None, "layer", "blk"),
        P(None, "blk"),
        P("layer", None),
        P("layer", "blk"),
        P("blk", None),
        P("blk"),
        P(),
        P(),
    )
    out_specs = P("layer", "blk")
    return jax.shard_map(
        on_device, mesh=mesh, in_specs=in_specs, out_specs=out_specs, check_vma=False
    )
```

```python
import functools

import jax
import jax.numpy as jnp
from jax import lax
from jax.experimental import pallas as pl
from jax.experimental.pallas import tpu as pltpu
from jax.sharding import PartitionSpec as P

MESH = pl.DeviceIdType.MESH
CHUNK = 512
NEAR = 2


def local_sums(weight, owner, local, owners, cells):
    types, patches = weight.shape
    chunk = CHUNK if patches % CHUNK == 0 else patches
    tall = 16
    rows = lax.broadcasted_iota(jnp.int32, (tall, chunk), 0) // types
    groups = owners * types // tall
    per = tall // types
    row_owner = [(rows + per * g).astype(jnp.int16) for g in range(groups)]
    cell = lax.broadcasted_iota(jnp.int32, (cells, chunk), 0).astype(jnp.int16)
    zero, one = jnp.bfloat16(0.0), jnp.bfloat16(1.0)
    total = None
    for start in range(0, patches, chunk):
        part = slice(start, start + chunk)
        w = weight[:, part]
        w = jnp.concatenate([w] * (8 // types), axis=0)
        high = w.astype(jnp.bfloat16).astype(jnp.float32)
        low = w - high
        high, low = [
            jnp.concatenate([piece] * (tall // 8), axis=0).astype(jnp.bfloat16)
            for piece in (high, low)
        ]
        who = jnp.broadcast_to(owner[:, part], (tall, chunk)).astype(jnp.int16)
        named = [row == who for row in row_owner]
        left = jnp.concatenate(
            [jnp.where(name, piece, zero) for piece in (high, low) for name in named], axis=0
        )
        where = jnp.broadcast_to(local[:, part], (tall, chunk)).astype(jnp.int16)
        where = jnp.concatenate([where] * (cells // tall), axis=0)
        table = jnp.where(cell == where, one, zero).astype(jnp.float8_e4m3fn)
        product = lax.dot_general(
            left, table, (((1,), (1,)), ((), ())), preferred_element_type=jnp.float32
        )
        total = product if total is None else total + product
    return total[: owners * types] + total[owners * types :]


def spread(value, out):
    out[...] = jnp.zeros(out.shape, out.dtype) + value[0].astype(out.dtype)


def blank(out):
    out[...] = jnp.zeros(out.shape, out.dtype)


def kernel(
    n, m, given, leaf_hbm, soil_hbm, root_hbm, weight_hbm, owner_hbm, local_hbm,
    out_ref, soil, root, weight, owner, local, leaf, scalars, sums, pairs, got,
    load_sem, send_sem, recv_sem, met_sem,
):
    blk, layer = lax.axis_index("blk"), lax.axis_index("layer")
    types, cells = out_ref.shape
    months = leaf.shape[1]
    everywhere = [(b, k) for b in range(n) for k in range(m)]
    is_near = jnp.logical_and(blk == 0, layer >= NEAR)
    pair_sem, leaf_sem, scalar_sem = n, n + 1, n + 2
    copies = [
        (weight_hbm, weight),
        (owner_hbm, owner),
        (local_hbm, local),
        (root_hbm, root),
        (soil_hbm, soil),
        (leaf_hbm, leaf.at[layer]),
    ]
    loads = [
        pltpu.make_async_copy(source, target, load_sem.at[i])
        for i, (source, target) in enumerate(copies)
    ]
    for load in loads:
        load.start()

    barrier = pltpu.get_barrier_semaphore()

    def greet(semaphore, b, k):
        pl.semaphore_signal(semaphore, inc=1, device_id=(b, k), device_id_type=MESH)

    peers = [lax.rem(layer + j, m) for j in range(1, m)]
    for k in peers:
        greet(barrier, blk, k)
    for b in range(n):

        @pl.when(blk != b)
        def _():
            for k in range(m if b else min(NEAR, m)):
                greet(barrier, b, k)

    got[blk] = jnp.zeros(got.shape[1:], got.dtype)
    for load in loads[3:5]:
        load.wait()
    stress = root[:, 0:1] * soil[0:1, :]
    for i in range(1, soil.shape[0]):
        stress += root[:, i : i + 1] * soil[i : i + 1, :]
    pairs[layer, 1] = stress
    for load in loads[:3]:
        load.wait()
    partial = local_sums(weight, owner, local, n, cells)
    for i in range(n):
        sums[i] = partial[i * types : (i + 1) * types]

    def send(source, target, sem, b, k):
        pltpu.make_async_remote_copy(
            src_ref=source,
            dst_ref=target,
            send_sem=send_sem.at[sem],
            recv_sem=recv_sem.at[sem],
            device_id=(b, k),
            device_id_type=MESH,
        ).start()

    def send_peers():
        for k in peers:
            send(pairs.at[layer], pairs.at[layer], pair_sem, blk, k)
        for k in peers:
            send(leaf.at[layer], leaf.at[layer], leaf_sem, blk, k)

    pl.semaphore_wait(barrier, jnp.where(is_near, m - 1, n * m - 1))

    @pl.when(is_near)
    def _():
        pairs[layer, 0] = sums[blk]
        loads[5].wait()
        send_peers()
        pl.semaphore_wait(met_sem, (n - 1) * m)

    for b in range(n):

        @pl.when(blk != b)
        def _():
            for k in range(m):
                send(sums.at[b], got.at[blk, layer], blk, b, k)
                if b == 0 and k >= NEAR:
                    greet(met_sem, b, k)

    @pl.when(jnp.logical_not(is_near))
    def _():
        pairs[layer, 0] = sums[blk]
        loads[5].wait()
        send_peers()

    reads = [jnp.logical_and(blk == 0, layer == k) for k in range(2)]
    for k, read in enumerate(reads):
        row = scalars.at[k]

        @pl.when(read)
        def _():
            for place in everywhere:
                if place != (0, k):
                    send(given, row, scalar_sem + k, *place)
            row[...] = given[...]

        @pl.when(jnp.logical_not(read))
        def _():
            pltpu.make_async_copy(row, row, recv_sem.at[scalar_sem + k]).wait()

    others = pl.ds(0, m - 1)
    arrivals = [(pairs.at[others], pair_sem), (leaf.at[others], leaf_sem)]
    for ref, sem in arrivals:
        pltpu.make_async_copy(ref, ref, recv_sem.at[sem]).wait()
    first, mix = scalars[0], scalars[1]
    second = jnp.where(first == months - 1, 0.0, first + 1.0)
    share = [
        jnp.where(first == k, mix, jnp.where(second == k, 1.0 - mix, 0.0)) for k in range(months)
    ]
    effects, grids = [], []
    for k in range(m):
        current = share[0] * leaf[k, 0]
        for i in range(1, months):
            current += share[i] * leaf[k, i]
        effects.append((1.0 - jnp.exp(-0.5 * current)) * pairs[k, 1])
        grids.append(pairs[k, 0])
    for b in range(n):
        if b == n - 1:
            sent = got.at[pl.ds(0, n - 1)]
            pltpu.make_async_copy(sent, sent, send_sem.at[blk]).wait()
            for ref, sem in arrivals:
                pltpu.make_async_copy(ref, ref, send_sem.at[sem]).wait()
            for k, read in enumerate(reads):
                row = scalars.at[k]

                @pl.when(read)
                def _():
                    for _ in everywhere[1:]:
                        pltpu.make_async_copy(row, row, send_sem.at[scalar_sem + k]).wait()

        @pl.when(blk != b)
        def _():
            pltpu.make_async_copy(got.at[b], got.at[b], recv_sem.at[b]).wait()

        grids = [grid + got[b, k] for k, grid in enumerate(grids)]
    mine, everyone = None, None
    for k in range(m):
        grid = grids[k] * effects[k]
        mine = grid if k == 0 else jnp.where(layer == k, grid, mine)
        everyone = grid if k == 0 else everyone + grid
    out_ref[...] = mine / (1.0 + jnp.sum(everyone, axis=0, keepdims=True))


def on_device(
    leaf_area, soil_water, root_share, patch_weight, patch_owner, patch_local, month, mix
):
    n, m = lax.axis_size("blk"), lax.axis_size("layer")
    months, types, cells = leaf_area.shape
    patches = patch_local.shape[0]
    owner = patch_owner.reshape(1, patches)
    local = patch_local.reshape(1, patches)
    f32, i32 = jnp.float32, jnp.int32
    hbm = pl.BlockSpec(memory_space=pl.ANY)
    vmem = pl.BlockSpec(memory_space=pltpu.VMEM)
    smem = pl.BlockSpec(memory_space=pltpu.SMEM)
    row = jax.ShapeDtypeStruct((1, cells), f32)

    def reader(value):
        return pl.pallas_call(spread, out_shape=row, in_specs=[smem], out_specs=vmem)(value)

    role = jnp.where(lax.axis_index("blk") == 0, jnp.minimum(lax.axis_index("layer"), 2), 2)
    given = lax.switch(
        role,
        [
            lambda month, mix: reader(month),
            lambda month, mix: reader(mix),
            lambda month, mix: pl.pallas_call(blank, out_shape=row, out_specs=vmem)(),
        ],
        month,
        mix,
    )
    return pl.pallas_call(
        functools.partial(kernel, n, m),
        out_shape=pltpu.VMEM((types, cells), f32),
        in_specs=[vmem] + [hbm] * 6,
        out_specs=vmem,
        scratch_shapes=[
            pltpu.VMEM(soil_water.shape, f32),
            pltpu.VMEM(root_share.shape, f32),
            pltpu.VMEM(patch_weight.shape, f32),
            pltpu.VMEM(owner.shape, i32),
            pltpu.VMEM(local.shape, i32),
            pltpu.VMEM((m, months, types, cells), f32),
            pltpu.VMEM((2, *row.shape), f32),
            pltpu.VMEM((n, types, cells), f32),
            pltpu.VMEM((m, 2, types, cells), f32),
            pltpu.VMEM((n, m, types, cells), f32),
            pltpu.SemaphoreType.DMA((6,)),
            pltpu.SemaphoreType.DMA((n + 4,)),
            pltpu.SemaphoreType.DMA((n + 4,)),
            pltpu.SemaphoreType.REGULAR,
        ],
        compiler_params=pltpu.CompilerParams(collective_id=0, has_side_effects=True),
    )(given, leaf_area, soil_water, root_share, patch_weight, owner, local)


def solution(mesh):
    in_specs = (
        P(None, "layer", "blk"),
        P(None, "blk"),
        P("layer", None),
        P("layer", "blk"),
        P("blk", None),
        P("blk"),
        P(),
        P(),
    )
    out_specs = P("layer", "blk")
    return jax.shard_map(
        on_device, mesh=mesh, in_specs=in_specs, out_specs=out_specs, check_vma=False
    )
```

```python
import functools

import jax
import jax.numpy as jnp
from jax import lax
from jax.experimental import pallas as pl
from jax.experimental.pallas import tpu as pltpu
from jax.sharding import PartitionSpec as P

MESH = pl.DeviceIdType.MESH
CHUNK = 512
NEAR = 2


def local_sums(weight, owner, local, owners, cells):
    types, patches = weight.shape
    chunk = CHUNK if patches % CHUNK == 0 else patches
    tall = 16
    rows = lax.broadcasted_iota(jnp.int32, (tall, chunk), 0) // types
    groups = owners * types // tall
    per = tall // types
    row_owner = [(rows + per * g).astype(jnp.int16) for g in range(groups)]
    cell = lax.broadcasted_iota(jnp.int32, (cells, chunk), 0).astype(jnp.int16)
    zero, one = jnp.bfloat16(0.0), jnp.bfloat16(1.0)
    total = None
    for start in range(0, patches, chunk):
        part = slice(start, start + chunk)
        w = weight[:, part]
        w = jnp.concatenate([w] * (8 // types), axis=0)
        high = w.astype(jnp.bfloat16).astype(jnp.float32)
        low = w - high
        high, low = [
            jnp.concatenate([piece] * (tall // 8), axis=0).astype(jnp.bfloat16)
            for piece in (high, low)
        ]
        who = jnp.broadcast_to(owner[:, part], (tall, chunk)).astype(jnp.int16)
        named = [row == who for row in row_owner]
        left = jnp.concatenate(
            [jnp.where(name, piece, zero) for piece in (high, low) for name in named], axis=0
        )
        where = jnp.broadcast_to(local[:, part], (tall, chunk)).astype(jnp.int16)
        where = jnp.concatenate([where] * (cells // tall), axis=0)
        table = jnp.where(cell == where, one, zero).astype(jnp.float8_e4m3fn)
        product = lax.dot_general(
            left, table, (((1,), (1,)), ((), ())), preferred_element_type=jnp.float32
        )
        total = product if total is None else total + product
    return total[: owners * types] + total[owners * types :]


def spread(value, out):
    out[...] = jnp.zeros(out.shape, out.dtype) + value[0].astype(out.dtype)


def blank(out):
    out[...] = jnp.zeros(out.shape, out.dtype)


def put_rows(share, out, sem):
    for i in range(share.shape[0]):
        row = pl.ds(i, 1)
        pltpu.make_async_copy(share.at[row], out.at[row], sem).start()
    pltpu.make_async_copy(share, out, sem).wait()


def kernel(
    n, m, given, leaf_hbm, soil_hbm, root_hbm, weight_hbm, owner_hbm, local_hbm,
    out_ref, soil, root, weight, owner, local, leaf, scalars, sums, pairs, got,
    tally, load_sem, side_sem, root_sem, send_sem, sum_sem, part_sem, met_sem,
):
    blk, layer = lax.axis_index("blk"), lax.axis_index("layer")
    types, cells = out_ref.shape
    months = leaf.shape[1]
    everywhere = [(b, k) for b in range(n) for k in range(m)]
    is_near = jnp.logical_and(blk == 0, layer >= NEAR)
    parts = (m - 1) * (2 + months) * types

    def settle(semaphore, rows):
        pltpu.make_async_copy(tally.at[pl.ds(0, rows)], tally.at[pl.ds(0, rows)], semaphore).wait()

    for source, target, semaphore in (
        (weight_hbm, weight, load_sem),
        (owner_hbm, owner, load_sem),
        (local_hbm, local, load_sem),
        (root_hbm, root, root_sem),
        (soil_hbm, soil, side_sem),
        (leaf_hbm, leaf.at[layer], side_sem),
    ):
        pltpu.make_async_copy(source, target, semaphore).start()

    barrier = pltpu.get_barrier_semaphore()

    def greet(semaphore, b, k):
        pl.semaphore_signal(semaphore, inc=1, device_id=(b, k), device_id_type=MESH)

    peers = [lax.rem(layer + j, m) for j in range(1, m)]
    for k in peers:
        greet(barrier, blk, k)
    for b in range(n):

        @pl.when(blk != b)
        def _():
            for k in range(m if b else min(NEAR, m)):
                greet(barrier, b, k)

    got[blk] = jnp.zeros(got.shape[1:], got.dtype)
    settle(load_sem, (types + 2) * weight.shape[1] // cells)
    partial = local_sums(weight, owner, local, n, cells)
    for i in range(n):
        sums[i] = partial[i * types : (i + 1) * types]

    def send(source, target, sem, b, k):
        pltpu.make_async_remote_copy(
            src_ref=source,
            dst_ref=target,
            send_sem=send_sem,
            recv_sem=sem,
            device_id=(b, k),
            device_id_type=MESH,
        ).start()

    def send_peers():
        pltpu.make_async_copy(root_hbm, root, root_sem).wait()
        settle(side_sem, soil.shape[0] + months * types)
        stress = root[:, 0:1] * soil[0:1, :]
        for i in range(1, soil.shape[0]):
            stress += root[:, i : i + 1] * soil[i : i + 1, :]
        pairs[layer, 0] = sums[blk]
        pairs[layer, 1] = stress
        for k in peers:
            send(pairs.at[layer], pairs.at[layer], part_sem, blk, k)
        for k in peers:
            send(leaf.at[layer], leaf.at[layer], part_sem, blk, k)

    pl.semaphore_wait(barrier, jnp.where(is_near, m - 1, n * m - 1))

    @pl.when(is_near)
    def _():
        send_peers()
        pl.semaphore_wait(met_sem, (n - 1) * m)

    for b in range(n):

        @pl.when(blk != b)
        def _():
            for k in range(m):
                send(sums.at[b], got.at[blk, layer], sum_sem, b, k)
                if b == 0 and k >= NEAR:
                    greet(met_sem, b, k)

    @pl.when(jnp.logical_not(is_near))
    def _():
        send_peers()

    reads = [jnp.logical_and(blk == 0, layer == k) for k in range(2)]
    for k, read in enumerate(reads):
        row = scalars.at[k]

        @pl.when(read)
        def _():
            for place in everywhere:
                if place != (0, k):
                    send(given, row, part_sem, *place)
            row[...] = given[...]

    is_reader = jnp.logical_or(*reads)
    pl.when(is_reader)(lambda: settle(part_sem, parts + 1))
    pl.when(jnp.logical_not(is_reader))(lambda: settle(part_sem, parts + 2))
    first, mix = scalars[0], scalars[1]
    second = jnp.where(first == months - 1, 0.0, first + 1.0)
    share = [
        jnp.where(first == k, mix, jnp.where(second == k, 1.0 - mix, 0.0)) for k in range(months)
    ]
    effects, grids = [], []
    for k in range(m):
        current = share[0] * leaf[k, 0]
        for i in range(1, months):
            current += share[i] * leaf[k, i]
        effects.append((1.0 - jnp.exp(-0.5 * current)) * pairs[k, 1])
        grids.append(pairs[k, 0])
    sent = (n - 1) * m * types + parts
    pl.when(is_reader)(lambda: settle(send_sem, sent + n * m - 1))
    pl.when(jnp.logical_not(is_reader))(lambda: settle(send_sem, sent))
    settle(sum_sem, (n - 1) * m * types)
    for b in range(n):
        grids = [grid + got[b, k] for k, grid in enumerate(grids)]
    mine, everyone = None, None
    for k in range(m):
        grid = grids[k] * effects[k]
        mine = grid if k == 0 else jnp.where(layer == k, grid, mine)
        everyone = grid if k == 0 else everyone + grid
    out_ref[...] = mine / (1.0 + jnp.sum(everyone, axis=0, keepdims=True))


def on_device(
    leaf_area, soil_water, root_share, patch_weight, patch_owner, patch_local, month, mix
):
    n, m = lax.axis_size("blk"), lax.axis_size("layer")
    months, types, cells = leaf_area.shape
    patches = patch_local.shape[0]
    owner = patch_owner.reshape(1, patches)
    local = patch_local.reshape(1, patches)
    f32, i32 = jnp.float32, jnp.int32
    hbm = pl.BlockSpec(memory_space=pl.ANY)
    vmem = pl.BlockSpec(memory_space=pltpu.VMEM)
    smem = pl.BlockSpec(memory_space=pltpu.SMEM)
    row = jax.ShapeDtypeStruct((1, cells), f32)
    rows = max(
        (types + 2) * patches // cells,
        (n - 1) * m * types + (m - 1) * (2 + months) * types + n * m,
        soil_water.shape[0] + months * types,
    )

    def reader(value):
        return pl.pallas_call(spread, out_shape=row, in_specs=[smem], out_specs=vmem)(value)

    role = jnp.where(lax.axis_index("blk") == 0, jnp.minimum(lax.axis_index("layer"), 2), 2)
    given = lax.switch(
        role,
        [
            lambda month, mix: reader(month),
            lambda month, mix: reader(mix),
            lambda month, mix: pl.pallas_call(blank, out_shape=row, out_specs=vmem)(),
        ],
        month,
        mix,
    )
    share = pl.pallas_call(
        functools.partial(kernel, n, m),
        out_shape=pltpu.VMEM((types, cells), f32),
        in_specs=[vmem] + [hbm] * 6,
        out_specs=vmem,
        scratch_shapes=[
            pltpu.VMEM(soil_water.shape, f32),
            pltpu.VMEM(root_share.shape, f32),
            pltpu.VMEM(patch_weight.shape, f32),
            pltpu.VMEM(owner.shape, i32),
            pltpu.VMEM(local.shape, i32),
            pltpu.VMEM((m, months, types, cells), f32),
            pltpu.VMEM((2, *row.shape), f32),
            pltpu.VMEM((n, types, cells), f32),
            pltpu.VMEM((m, 2, types, cells), f32),
            pltpu.VMEM((n, m, types, cells), f32),
            pltpu.VMEM((rows, cells), f32),
            *[pltpu.SemaphoreType.DMA] * 6,
            pltpu.SemaphoreType.REGULAR,
        ],
        compiler_params=pltpu.CompilerParams(collective_id=0, has_side_effects=True),
    )(given, leaf_area, soil_water, root_share, patch_weight, owner, local)
    return pl.pallas_call(
        put_rows,
        out_shape=jax.ShapeDtypeStruct(share.shape, f32),
        in_specs=[vmem],
        out_specs=hbm,
        scratch_shapes=[pltpu.SemaphoreType.DMA],
    )(pltpu.with_memory_space_constraint(share, pltpu.VMEM))


def solution(mesh):
    in_specs = (
        P(None, "layer", "blk"),
        P(None, "blk"),
        P("layer", None),
        P("layer", "blk"),
        P("blk", None),
        P("blk"),
        P(),
        P(),
    )
    out_specs = P("layer", "blk")
    return jax.shard_map(
        on_device, mesh=mesh, in_specs=in_specs, out_specs=out_specs, check_vma=False
    )
```

```python
import functools

import jax
import jax.numpy as jnp
from jax import lax
from jax.experimental import pallas as pl
from jax.experimental.pallas import tpu as pltpu
from jax.sharding import PartitionSpec as P

MESH = pl.DeviceIdType.MESH
CHUNK = 512
NEAR = 2


def local_sums(weight, owner, local, owners, cells):
    types, patches = weight.shape
    chunk = CHUNK if patches % CHUNK == 0 else patches
    tall = 16
    rows = lax.broadcasted_iota(jnp.int32, (tall, chunk), 0) // types
    groups = owners * types // tall
    per = tall // types
    row_owner = [(rows + per * g).astype(jnp.int16) for g in range(groups)]
    cell = lax.broadcasted_iota(jnp.int32, (cells, chunk), 0).astype(jnp.int16)
    zero, one = jnp.bfloat16(0.0), jnp.bfloat16(1.0)
    total = None
    for start in range(0, patches, chunk):
        part = slice(start, start + chunk)
        w = weight[:, part]
        w = jnp.concatenate([w] * (8 // types), axis=0)
        high = w.astype(jnp.bfloat16).astype(jnp.float32)
        low = w - high
        high, low = [
            jnp.concatenate([piece] * (tall // 8), axis=0).astype(jnp.bfloat16)
            for piece in (high, low)
        ]
        who = jnp.broadcast_to(owner[:, part], (tall, chunk)).astype(jnp.int16)
        named = [row == who for row in row_owner]
        left = jnp.concatenate(
            [jnp.where(name, piece, zero) for piece in (high, low) for name in named], axis=0
        )
        where = jnp.broadcast_to(local[:, part], (tall, chunk)).astype(jnp.int16)
        where = jnp.concatenate([where] * (cells // tall), axis=0)
        table = jnp.where(cell == where, one, zero).astype(jnp.float8_e4m3fn)
        product = lax.dot_general(
            left, table, (((1,), (1,)), ((), ())), preferred_element_type=jnp.float32
        )
        total = product if total is None else total + product
    return total[: owners * types] + total[owners * types :]


def spread(value, out):
    out[...] = jnp.zeros(out.shape, out.dtype) + value[0].astype(out.dtype)


def blank(out):
    out[...] = jnp.zeros(out.shape, out.dtype)


def put_rows(share, out):
    def body(sem):
        for i in range(share.shape[0]):
            row = pl.ds(i, 1)
            pltpu.make_async_copy(share.at[row], out.at[row], sem).start()
        pltpu.make_async_copy(share, out, sem).wait()

    pl.run_scoped(body, pltpu.SemaphoreType.DMA)


def kernel(
    n, m, given, leaf_hbm, soil_hbm, root_hbm, weight_hbm, owner_hbm, local_hbm,
    out_ref, soil, root, weight, owner, local, leaf, scalars, sums, pairs, got,
    tally, sum_sem, part_sem, met_sem,
):
    def body(load_sem, side_sem, root_sem, send_sem):
        exchange(
            n, m, given, leaf_hbm, soil_hbm, root_hbm, weight_hbm, owner_hbm, local_hbm,
            out_ref, soil, root, weight, owner, local, leaf, scalars, sums, pairs, got,
            tally, load_sem, side_sem, root_sem, send_sem, sum_sem, part_sem, met_sem,
        )

    pl.run_scoped(body, *[pltpu.SemaphoreType.DMA] * 4)


def exchange(
    n, m, given, leaf_hbm, soil_hbm, root_hbm, weight_hbm, owner_hbm, local_hbm,
    out_ref, soil, root, weight, owner, local, leaf, scalars, sums, pairs, got,
    tally, load_sem, side_sem, root_sem, send_sem, sum_sem, part_sem, met_sem,
):
    blk, layer = lax.axis_index("blk"), lax.axis_index("layer")
    types, cells = out_ref.shape
    months = leaf.shape[1]
    everywhere = [(b, k) for b in range(n) for k in range(m)]
    is_near = jnp.logical_and(blk == 0, layer >= NEAR)
    parts = (m - 1) * (2 + months) * types

    def settle(semaphore, rows):
        pltpu.make_async_copy(tally.at[pl.ds(0, rows)], tally.at[pl.ds(0, rows)], semaphore).wait()

    for source, target, semaphore in (
        (weight_hbm, weight, load_sem),
        (owner_hbm, owner, load_sem),
        (local_hbm, local, load_sem),
        (root_hbm, root, root_sem),
        (soil_hbm, soil, side_sem),
        (leaf_hbm, leaf.at[layer], side_sem),
    ):
        pltpu.make_async_copy(source, target, semaphore).start()

    barrier = pltpu.get_barrier_semaphore()

    def greet(semaphore, b, k):
        pl.semaphore_signal(semaphore, inc=1, device_id=(b, k), device_id_type=MESH)

    peers = [lax.rem(layer + j, m) for j in range(1, m)]
    for k in peers:
        greet(barrier, blk, k)
    for b in reversed(range(n)):

        @pl.when(blk != b)
        def _():
            for k in range(m if b else min(NEAR, m)):
                greet(barrier, b, k)

    got[blk] = jnp.zeros(got.shape[1:], got.dtype)
    settle(load_sem, (types + 2) * weight.shape[1] // cells)
    partial = local_sums(weight, owner, local, n, cells)
    for i in range(n):
        sums[i] = partial[i * types : (i + 1) * types]

    def send(source, target, sem, b, k):
        pltpu.make_async_remote_copy(
            src_ref=source,
            dst_ref=target,
            send_sem=send_sem,
            recv_sem=sem,
            device_id=(b, k),
            device_id_type=MESH,
        ).start()

    def send_peers():
        pltpu.make_async_copy(root_hbm, root, root_sem).wait()
        settle(side_sem, soil.shape[0] + months * types)
        stress = root[:, 0:1] * soil[0:1, :]
        for i in range(1, soil.shape[0]):
            stress += root[:, i : i + 1] * soil[i : i + 1, :]
        pairs[layer, 0] = sums[blk]
        pairs[layer, 1] = stress
        for k in peers:
            send(pairs.at[layer], pairs.at[layer], part_sem, blk, k)
        for k in peers:
            send(leaf.at[layer], leaf.at[layer], part_sem, blk, k)

    pl.semaphore_wait(barrier, jnp.where(is_near, m - 1, n * m - 1))

    @pl.when(is_near)
    def _():
        send_peers()
        pl.semaphore_wait(met_sem, (n - 1) * m)

    for b in range(n):

        @pl.when(blk != b)
        def _():
            for k in range(m):
                send(sums.at[b], got.at[blk, layer], sum_sem, b, k)
                if b == 0 and k >= NEAR:
                    greet(met_sem, b, k)

    @pl.when(jnp.logical_not(is_near))
    def _():
        send_peers()

    reads = [jnp.logical_and(blk == 0, layer == k) for k in range(2)]
    for k, read in enumerate(reads):
        row = scalars.at[k]

        @pl.when(read)
        def _():
            for place in everywhere:
                if place != (0, k):
                    send(given, row, part_sem, *place)
            row[...] = given[...]

    is_reader = jnp.logical_or(*reads)
    pl.when(is_reader)(lambda: settle(part_sem, parts + 1))
    pl.when(jnp.logical_not(is_reader))(lambda: settle(part_sem, parts + 2))
    first, mix = scalars[0], scalars[1]
    second = jnp.where(first == months - 1, 0.0, first + 1.0)
    share = [
        jnp.where(first == k, mix, jnp.where(second == k, 1.0 - mix, 0.0)) for k in range(months)
    ]
    effects, grids = [], []
    for k in range(m):
        current = share[0] * leaf[k, 0]
        for i in range(1, months):
            current += share[i] * leaf[k, i]
        effects.append((1.0 - jnp.exp(-0.5 * current)) * pairs[k, 1])
        grids.append(pairs[k, 0])
    sent = (n - 1) * m * types + parts
    pl.when(is_reader)(lambda: settle(send_sem, sent + n * m - 1))
    pl.when(jnp.logical_not(is_reader))(lambda: settle(send_sem, sent))
    settle(sum_sem, (n - 1) * m * types)
    for b in range(n):
        grids = [grid + got[b, k] for k, grid in enumerate(grids)]
    mine, everyone = None, None
    for k in range(m):
        grid = grids[k] * effects[k]
        mine = grid if k == 0 else jnp.where(layer == k, grid, mine)
        everyone = grid if k == 0 else everyone + grid
    out_ref[...] = mine / (1.0 + jnp.sum(everyone, axis=0, keepdims=True))


def on_device(
    leaf_area, soil_water, root_share, patch_weight, patch_owner, patch_local, month, mix
):
    n, m = lax.axis_size("blk"), lax.axis_size("layer")
    months, types, cells = leaf_area.shape
    patches = patch_local.shape[0]
    owner = patch_owner.reshape(1, patches)
    local = patch_local.reshape(1, patches)
    f32, i32 = jnp.float32, jnp.int32
    hbm = pl.BlockSpec(memory_space=pl.ANY)
    vmem = pl.BlockSpec(memory_space=pltpu.VMEM)
    smem = pl.BlockSpec(memory_space=pltpu.SMEM)
    row = jax.ShapeDtypeStruct((1, cells), f32)
    rows = max(
        (types + 2) * patches // cells,
        (n - 1) * m * types + (m - 1) * (2 + months) * types + n * m,
        soil_water.shape[0] + months * types,
    )

    def reader(value):
        return pl.pallas_call(spread, out_shape=row, in_specs=[smem], out_specs=vmem)(value)

    role = jnp.where(lax.axis_index("blk") == 0, jnp.minimum(lax.axis_index("layer"), 2), 2)
    given = lax.switch(
        role,
        [
            lambda month, mix: reader(month),
            lambda month, mix: reader(mix),
            lambda month, mix: pl.pallas_call(blank, out_shape=row, out_specs=vmem)(),
        ],
        month,
        mix,
    )
    share = pl.pallas_call(
        functools.partial(kernel, n, m),
        out_shape=pltpu.VMEM((types, cells), f32),
        in_specs=[vmem] + [hbm] * 6,
        out_specs=vmem,
        scratch_shapes=[
            pltpu.VMEM(soil_water.shape, f32),
            pltpu.VMEM(root_share.shape, f32),
            pltpu.VMEM(patch_weight.shape, f32),
            pltpu.VMEM(owner.shape, i32),
            pltpu.VMEM(local.shape, i32),
            pltpu.VMEM((m, months, types, cells), f32),
            pltpu.VMEM((2, *row.shape), f32),
            pltpu.VMEM((n, types, cells), f32),
            pltpu.VMEM((m, 2, types, cells), f32),
            pltpu.VMEM((n, m, types, cells), f32),
            pltpu.VMEM((rows, cells), f32),
            *[pltpu.SemaphoreType.DMA] * 2,
            pltpu.SemaphoreType.REGULAR,
        ],
        compiler_params=pltpu.CompilerParams(collective_id=0, has_side_effects=True),
    )(given, leaf_area, soil_water, root_share, patch_weight, owner, local)
    return pl.pallas_call(
        put_rows,
        out_shape=jax.ShapeDtypeStruct(share.shape, f32),
        in_specs=[vmem],
        out_specs=hbm,
    )(pltpu.with_memory_space_constraint(share, pltpu.VMEM))


def solution(mesh):
    in_specs = (
        P(None, "layer", "blk"),
        P(None, "blk"),
        P("layer", None),
        P("layer", "blk"),
        P("blk", None),
        P("blk"),
        P(),
        P(),
    )
    out_specs = P("layer", "blk")
    return jax.shard_map(
        on_device, mesh=mesh, in_specs=in_specs, out_specs=out_specs, check_vma=False
    )
```

```python
import functools

import jax
import jax.numpy as jnp
from jax import lax
from jax.experimental import pallas as pl
from jax.experimental.pallas import tpu as pltpu
from jax.sharding import PartitionSpec as P

MESH = pl.DeviceIdType.MESH
CHUNK = 512
NEAR = 2


def local_sums(weight, owner, local, owners, cells):
    types, patches = weight.shape
    chunk = CHUNK if patches % CHUNK == 0 else patches
    tall = 16
    rows = lax.broadcasted_iota(jnp.int32, (tall, chunk), 0) // types
    groups = owners * types // tall
    per = tall // types
    row_owner = [(rows + per * g).astype(jnp.int16) for g in range(groups)]
    cell = lax.broadcasted_iota(jnp.int32, (cells, chunk), 0).astype(jnp.int16)
    zero, one = jnp.bfloat16(0.0), jnp.bfloat16(1.0)
    total = None
    for start in range(0, patches, chunk):
        part = slice(start, start + chunk)
        w = weight[:, part]
        w = jnp.concatenate([w] * (8 // types), axis=0)
        high = w.astype(jnp.bfloat16).astype(jnp.float32)
        low = w - high
        high, low = [
            jnp.concatenate([piece] * (tall // 8), axis=0).astype(jnp.bfloat16)
            for piece in (high, low)
        ]
        who = jnp.broadcast_to(owner[:, part], (tall, chunk)).astype(jnp.int16)
        named = [row == who for row in row_owner]
        left = jnp.concatenate(
            [jnp.where(name, piece, zero) for piece in (high, low) for name in named], axis=0
        )
        where = jnp.broadcast_to(local[:, part], (tall, chunk)).astype(jnp.int16)
        where = jnp.concatenate([where] * (cells // tall), axis=0)
        table = jnp.where(cell == where, one, zero).astype(jnp.float8_e4m3fn)
        product = lax.dot_general(
            left, table, (((1,), (1,)), ((), ())), preferred_element_type=jnp.float32
        )
        total = product if total is None else total + product
    return total[: owners * types] + total[owners * types :]


def spread(value, out):
    out[...] = jnp.zeros(out.shape, out.dtype) + value[0].astype(out.dtype)


def blank(out):
    out[...] = jnp.zeros(out.shape, out.dtype)


def put_rows(share, out):
    def body(sem):
        for i in range(share.shape[0]):
            row = pl.ds(i, 1)
            pltpu.make_async_copy(share.at[row], out.at[row], sem).start()
        pltpu.make_async_copy(share, out, sem).wait()

    pl.run_scoped(body, pltpu.SemaphoreType.DMA)


def kernel(
    n, m, given, leaf_hbm, soil_hbm, root_hbm, weight_hbm, owner_hbm, local_hbm,
    out_ref, soil, root, weight, owner, local, leaf, scalars, sums, pairs, got,
    tally, sum_sem, part_sem, met_sem,
):
    def body(load_sem, side_sem, root_sem, send_sem):
        exchange(
            n, m, given, leaf_hbm, soil_hbm, root_hbm, weight_hbm, owner_hbm, local_hbm,
            out_ref, soil, root, weight, owner, local, leaf, scalars, sums, pairs, got,
            tally, load_sem, side_sem, root_sem, send_sem, sum_sem, part_sem, met_sem,
        )

    pl.run_scoped(body, *[pltpu.SemaphoreType.DMA] * 4)


def exchange(
    n, m, given, leaf_hbm, soil_hbm, root_hbm, weight_hbm, owner_hbm, local_hbm,
    out_ref, soil, root, weight, owner, local, leaf, scalars, sums, pairs, got,
    tally, load_sem, side_sem, root_sem, send_sem, sum_sem, part_sem, met_sem,
):
    blk, layer = lax.axis_index("blk"), lax.axis_index("layer")
    types, cells = out_ref.shape
    months = leaf.shape[1]
    everywhere = [(b, k) for b in range(n) for k in range(m)]
    is_near = jnp.logical_and(blk == 0, layer >= NEAR)
    parts = (m - 1) * (2 + months) * types

    def settle(semaphore, rows):
        pltpu.make_async_copy(tally.at[pl.ds(0, rows)], tally.at[pl.ds(0, rows)], semaphore).wait()

    half = weight.shape[1] // 2
    for i, (source, target, semaphore) in enumerate((
        (weight_hbm.at[:, pl.ds(0, half)], weight.at[:, pl.ds(0, half)], load_sem),
        (weight_hbm.at[:, pl.ds(half, half)], weight.at[:, pl.ds(half, half)], load_sem),
        (owner_hbm, owner, load_sem),
        (local_hbm, local, load_sem),
        (root_hbm, root, root_sem),
        (soil_hbm, soil, side_sem),
        (leaf_hbm, leaf.at[layer], side_sem),
    )):
        pltpu.make_async_copy(source, target, semaphore).start(priority=i % 2)

    barrier = pltpu.get_barrier_semaphore()

    def greet(semaphore, b, k):
        pl.semaphore_signal(semaphore, inc=1, device_id=(b, k), device_id_type=MESH)

    peers = [lax.rem(layer + j, m) for j in range(1, m)]
    for k in peers:
        greet(barrier, blk, k)
    for b in reversed(range(n)):

        @pl.when(blk != b)
        def _():
            for k in range(m if b else min(NEAR, m)):
                greet(barrier, b, k)

    got[blk] = jnp.zeros(got.shape[1:], got.dtype)
    settle(load_sem, (types + 2) * weight.shape[1] // cells)
    partial = local_sums(weight, owner, local, n, cells)
    for i in range(n):
        sums[i] = partial[i * types : (i + 1) * types]

    def send(source, target, sem, b, k):
        pltpu.make_async_remote_copy(
            src_ref=source,
            dst_ref=target,
            send_sem=send_sem,
            recv_sem=sem,
            device_id=(b, k),
            device_id_type=MESH,
        ).start()

    def send_peers():
        pltpu.make_async_copy(root_hbm, root, root_sem).wait()
        settle(side_sem, soil.shape[0] + months * types)
        stress = root[:, 0:1] * soil[0:1, :]
        for i in range(1, soil.shape[0]):
            stress += root[:, i : i + 1] * soil[i : i + 1, :]
        pairs[layer, 0] = sums[blk]
        pairs[layer, 1] = stress
        for k in peers:
            send(pairs.at[layer], pairs.at[layer], part_sem, blk, k)
        for k in peers:
            send(leaf.at[layer], leaf.at[layer], part_sem, blk, k)

    pl.semaphore_wait(barrier, jnp.where(is_near, m - 1, n * m - 1))

    def send_sums(b):
        for k in range(m):
            send(sums.at[b], got.at[blk, layer], sum_sem, b, k)
            if b == 0 and k >= NEAR:
                greet(met_sem, b, k)

    pl.when(blk != 0)(functools.partial(send_sums, 0))

    @pl.when(is_near)
    def _():
        send_peers()
        pl.semaphore_wait(met_sem, (n - 1) * m)

    for b in range(1, n):
        pl.when(blk != b)(functools.partial(send_sums, b))

    @pl.when(jnp.logical_not(is_near))
    def _():
        send_peers()

    reads = [jnp.logical_and(blk == 0, layer == k) for k in range(2)]
    for k, read in enumerate(reads):
        row = scalars.at[k]

        @pl.when(read)
        def _():
            for place in everywhere:
                if place != (0, k):
                    send(given, row, part_sem, *place)
            row[...] = given[...]

    is_reader = jnp.logical_or(*reads)
    pl.when(is_reader)(lambda: settle(part_sem, parts + 1))
    pl.when(jnp.logical_not(is_reader))(lambda: settle(part_sem, parts + 2))
    first, mix = scalars[0], scalars[1]
    second = jnp.where(first == months - 1, 0.0, first + 1.0)
    share = [
        jnp.where(first == k, mix, jnp.where(second == k, 1.0 - mix, 0.0)) for k in range(months)
    ]
    effects, grids = [], []
    for k in range(m):
        current = share[0] * leaf[k, 0]
        for i in range(1, months):
            current += share[i] * leaf[k, i]
        effects.append((1.0 - jnp.exp(-0.5 * current)) * pairs[k, 1])
        grids.append(pairs[k, 0])
    sent = (n - 1) * m * types + parts
    pl.when(is_reader)(lambda: settle(send_sem, sent + n * m - 1))
    pl.when(jnp.logical_not(is_reader))(lambda: settle(send_sem, sent))
    settle(sum_sem, (n - 1) * m * types)
    for b in range(n):
        grids = [grid + got[b, k] for k, grid in enumerate(grids)]
    mine, everyone = None, None
    for k in range(m):
        grid = grids[k] * effects[k]
        mine = grid if k == 0 else jnp.where(layer == k, grid, mine)
        everyone = grid if k == 0 else everyone + grid
    out_ref[...] = mine / (1.0 + jnp.sum(everyone, axis=0, keepdims=True))


def on_device(
    leaf_area, soil_water, root_share, patch_weight, patch_owner, patch_local, month, mix
):
    n, m = lax.axis_size("blk"), lax.axis_size("layer")
    months, types, cells = leaf_area.shape
    patches = patch_local.shape[0]
    owner = patch_owner.reshape(1, patches)
    local = patch_local.reshape(1, patches)
    f32, i32 = jnp.float32, jnp.int32
    hbm = pl.BlockSpec(memory_space=pl.ANY)
    vmem = pl.BlockSpec(memory_space=pltpu.VMEM)
    smem = pl.BlockSpec(memory_space=pltpu.SMEM)
    row = jax.ShapeDtypeStruct((1, cells), f32)
    rows = max(
        (types + 2) * patches // cells,
        (n - 1) * m * types + (m - 1) * (2 + months) * types + n * m,
        soil_water.shape[0] + months * types,
    )

    def reader(value):
        return pl.pallas_call(spread, out_shape=row, in_specs=[smem], out_specs=vmem)(value)

    role = jnp.where(lax.axis_index("blk") == 0, jnp.minimum(lax.axis_index("layer"), 2), 2)
    given = lax.switch(
        role,
        [
            lambda month, mix: reader(month),
            lambda month, mix: reader(mix),
            lambda month, mix: pl.pallas_call(blank, out_shape=row, out_specs=vmem)(),
        ],
        month,
        mix,
    )
    share = pl.pallas_call(
        functools.partial(kernel, n, m),
        out_shape=pltpu.VMEM((types, cells), f32),
        in_specs=[vmem] + [hbm] * 6,
        out_specs=vmem,
        scratch_shapes=[
            pltpu.VMEM(soil_water.shape, f32),
            pltpu.VMEM(root_share.shape, f32),
            pltpu.VMEM(patch_weight.shape, f32),
            pltpu.VMEM(owner.shape, i32),
            pltpu.VMEM(local.shape, i32),
            pltpu.VMEM((m, months, types, cells), f32),
            pltpu.VMEM((2, *row.shape), f32),
            pltpu.VMEM((n, types, cells), f32),
            pltpu.VMEM((m, 2, types, cells), f32),
            pltpu.VMEM((n, m, types, cells), f32),
            pltpu.VMEM((rows, cells), f32),
            *[pltpu.SemaphoreType.DMA] * 2,
            pltpu.SemaphoreType.REGULAR,
        ],
        compiler_params=pltpu.CompilerParams(collective_id=0, has_side_effects=True),
    )(given, leaf_area, soil_water, root_share, patch_weight, owner, local)
    return pl.pallas_call(
        put_rows,
        out_shape=jax.ShapeDtypeStruct(share.shape, f32),
        in_specs=[vmem],
        out_specs=hbm,
    )(pltpu.with_memory_space_constraint(share, pltpu.VMEM))


def solution(mesh):
    in_specs = (
        P(None, "layer", "blk"),
        P(None, "blk"),
        P("layer", None),
        P("layer", "blk"),
        P("blk", None),
        P("blk"),
        P(),
        P(),
    )
    out_specs = P("layer", "blk")
    return jax.shard_map(
        on_device, mesh=mesh, in_specs=in_specs, out_specs=out_specs, check_vma=False
    )
```

```python
import functools

import jax
import jax.numpy as jnp
from jax import lax
from jax.experimental import pallas as pl
from jax.experimental.pallas import tpu as pltpu
from jax.sharding import PartitionSpec as P

MESH = pl.DeviceIdType.MESH
CHUNK = 512
NEAR = 2


def local_sums(weight, owner, local, owners, cells):
    types, patches = weight.shape
    chunk = CHUNK if patches % CHUNK == 0 else patches
    tall = 16
    rows = lax.broadcasted_iota(jnp.int32, (tall, chunk), 0) // types
    groups = owners * types // tall
    per = tall // types
    row_owner = [(rows + per * g).astype(jnp.int16) for g in range(groups)]
    cell = lax.broadcasted_iota(jnp.int32, (cells, chunk), 0).astype(jnp.int16)
    zero, one = jnp.bfloat16(0.0), jnp.bfloat16(1.0)
    total = None
    for start in range(0, patches, chunk):
        part = slice(start, start + chunk)
        w = weight[:, part]
        w = jnp.concatenate([w] * (8 // types), axis=0)
        high = w.astype(jnp.bfloat16).astype(jnp.float32)
        low = w - high
        high, low = [
            jnp.concatenate([piece] * (tall // 8), axis=0).astype(jnp.bfloat16)
            for piece in (high, low)
        ]
        who = jnp.broadcast_to(owner[:, part], (tall, chunk)).astype(jnp.int16)
        named = [row == who for row in row_owner]
        left = jnp.concatenate(
            [jnp.where(name, piece, zero) for piece in (high, low) for name in named], axis=0
        )
        where = jnp.broadcast_to(local[:, part], (tall, chunk)).astype(jnp.int16)
        where = jnp.concatenate([where] * (cells // tall), axis=0)
        table = jnp.where(cell == where, one, zero).astype(jnp.float8_e4m3fn)
        product = lax.dot_general(
            left, table, (((1,), (1,)), ((), ())), preferred_element_type=jnp.float32
        )
        total = product if total is None else total + product
    return total[: owners * types] + total[owners * types :]


def spread(value, out):
    out[...] = jnp.zeros(out.shape, out.dtype) + value[0].astype(out.dtype)


def blank(out):
    out[...] = jnp.zeros(out.shape, out.dtype)


def put_rows(share, out):
    def body(sem):
        for i in range(share.shape[0]):
            row = pl.ds(i, 1)
            pltpu.make_async_copy(share.at[row], out.at[row], sem).start()
        pltpu.make_async_copy(share, out, sem).wait()

    pl.run_scoped(body, pltpu.SemaphoreType.DMA)


def kernel(
    n, m, given, leaf_hbm, soil_hbm, root_hbm, weight_hbm, owner_hbm, local_hbm,
    out_ref, soil, root, weight, owner, local, leaf, scalars, sums, pairs, got,
    tally, sum_sem, part_sem, met_sem,
):
    def body(load_sem, side_sem, root_sem, send_sem):
        exchange(
            n, m, given, leaf_hbm, soil_hbm, root_hbm, weight_hbm, owner_hbm, local_hbm,
            out_ref, soil, root, weight, owner, local, leaf, scalars, sums, pairs, got,
            tally, load_sem, side_sem, root_sem, send_sem, sum_sem, part_sem, met_sem,
        )

    pl.run_scoped(body, *[pltpu.SemaphoreType.DMA] * 4)


def exchange(
    n, m, given, leaf_hbm, soil_hbm, root_hbm, weight_hbm, owner_hbm, local_hbm,
    out_ref, soil, root, weight, owner, local, leaf, scalars, sums, pairs, got,
    tally, load_sem, side_sem, root_sem, send_sem, sum_sem, part_sem, met_sem,
):
    blk, layer = lax.axis_index("blk"), lax.axis_index("layer")
    types, cells = out_ref.shape
    months = leaf.shape[1]
    everywhere = [(b, k) for b in range(n) for k in range(m)]
    is_near = jnp.logical_and(blk == 0, layer >= NEAR)
    parts = (m - 1) * (2 + months) * types

    def settle(semaphore, rows):
        pltpu.make_async_copy(tally.at[pl.ds(0, rows)], tally.at[pl.ds(0, rows)], semaphore).wait()

    half = weight.shape[1] // 2
    for i, (source, target, semaphore) in enumerate((
        (weight_hbm.at[:, pl.ds(0, half)], weight.at[:, pl.ds(0, half)], load_sem),
        (weight_hbm.at[:, pl.ds(half, half)], weight.at[:, pl.ds(half, half)], load_sem),
        (owner_hbm, owner, load_sem),
        (local_hbm, local, load_sem),
        (root_hbm, root, root_sem),
        (soil_hbm, soil, side_sem),
        (leaf_hbm, leaf.at[layer], side_sem),
    )):
        pltpu.make_async_copy(source, target, semaphore).start(priority=i % 2)

    barrier = pltpu.get_barrier_semaphore()

    def greet(semaphore, b, k):
        pl.semaphore_signal(semaphore, inc=1, device_id=(b, k), device_id_type=MESH)

    peers = [lax.rem(layer + j, m) for j in range(1, m)]
    for k in peers:
        greet(barrier, blk, k)
    for b in reversed(range(n)):

        @pl.when(blk != b)
        def _():
            for k in range(m if b else min(NEAR, m)):
                greet(barrier, b, k)

    got[blk] = jnp.zeros(got.shape[1:], got.dtype)
    settle(load_sem, (types + 2) * weight.shape[1] // cells)
    partial = local_sums(weight, owner, local, n, cells)
    for i in range(n):
        sums[i] = partial[i * types : (i + 1) * types]

    def send(source, target, sem, b, k):
        pltpu.make_async_remote_copy(
            src_ref=source,
            dst_ref=target,
            send_sem=send_sem,
            recv_sem=sem,
            device_id=(b, k),
            device_id_type=MESH,
        ).start()

    def send_peers():
        pltpu.make_async_copy(root_hbm, root, root_sem).wait()
        settle(side_sem, soil.shape[0] + months * types)
        stress = root[:, 0:1] * soil[0:1, :]
        for i in range(1, soil.shape[0]):
            stress += root[:, i : i + 1] * soil[i : i + 1, :]
        pairs[layer, 0] = sums[blk]
        pairs[layer, 1] = stress
        for k in peers:
            send(pairs.at[layer], pairs.at[layer], part_sem, blk, k)
        for k in peers:
            send(leaf.at[layer], leaf.at[layer], part_sem, blk, k)

    pl.semaphore_wait(barrier, jnp.where(is_near, m - 1, n * m - 1))

    def send_sums(b):
        for k in range(m):
            send(sums.at[b], got.at[blk, layer], sum_sem, b, k)
            if b == 0 and k >= NEAR:
                greet(met_sem, b, k)

    pl.when(blk != 0)(functools.partial(send_sums, 0))

    @pl.when(is_near)
    def _():
        send_peers()
        pl.semaphore_wait(met_sem, (n - 1) * m)

    for b in range(1, n):
        pl.when(blk != b)(functools.partial(send_sums, b))

    @pl.when(jnp.logical_not(is_near))
    def _():
        send_peers()

    reads = [jnp.logical_and(blk == 0, layer == k) for k in range(2)]
    for k, read in enumerate(reads):
        row = scalars.at[k]

        @pl.when(read)
        def _():
            for place in everywhere:
                if place != (0, k):
                    send(given, row, part_sem, *place)
            row[...] = given[...]

    is_reader = jnp.logical_or(*reads)
    pl.when(is_reader)(lambda: settle(part_sem, parts + 1))
    pl.when(jnp.logical_not(is_reader))(lambda: settle(part_sem, parts + 2))
    first, mix = scalars[0], scalars[1]
    second = jnp.where(first == months - 1, 0.0, first + 1.0)
    share = [
        jnp.where(first == k, mix, jnp.where(second == k, 1.0 - mix, 0.0)) for k in range(months)
    ]
    effects, grids = [], []
    for k in range(m):
        current = share[0] * leaf[k, 0]
        for i in range(1, months):
            current += share[i] * leaf[k, i]
        effects.append((1.0 - jnp.exp(-0.5 * current)) * pairs[k, 1])
        grids.append(pairs[k, 0])
    sent = (n - 1) * m * types + parts
    pl.when(is_reader)(lambda: settle(send_sem, sent + n * m - 1))
    pl.when(jnp.logical_not(is_reader))(lambda: settle(send_sem, sent))
    settle(sum_sem, (n - 1) * m * types)
    for k in range(m):
        terms = [grids[k]] + [got[b, k] for b in range(n)]
        while len(terms) > 1:
            terms = [sum(terms[i + 1 : i + 2], terms[i]) for i in range(0, len(terms), 2)]
        grids[k] = terms[0]
    mine, everyone = None, None
    for k in range(m):
        grid = grids[k] * effects[k]
        mine = grid if k == 0 else jnp.where(layer == k, grid, mine)
        everyone = grid if k == 0 else everyone + grid
    out_ref[...] = mine / (1.0 + jnp.sum(everyone, axis=0, keepdims=True))


def on_device(
    leaf_area, soil_water, root_share, patch_weight, patch_owner, patch_local, month, mix
):
    n, m = lax.axis_size("blk"), lax.axis_size("layer")
    months, types, cells = leaf_area.shape
    patches = patch_local.shape[0]
    owner = patch_owner.reshape(1, patches)
    local = patch_local.reshape(1, patches)
    f32, i32 = jnp.float32, jnp.int32
    hbm = pl.BlockSpec(memory_space=pl.ANY)
    vmem = pl.BlockSpec(memory_space=pltpu.VMEM)
    smem = pl.BlockSpec(memory_space=pltpu.SMEM)
    row = jax.ShapeDtypeStruct((1, cells), f32)
    rows = max(
        (types + 2) * patches // cells,
        (n - 1) * m * types + (m - 1) * (2 + months) * types + n * m,
        soil_water.shape[0] + months * types,
    )

    def reader(value):
        return pl.pallas_call(spread, out_shape=row, in_specs=[smem], out_specs=vmem)(value)

    role = jnp.where(lax.axis_index("blk") == 0, jnp.minimum(lax.axis_index("layer"), 2), 2)
    given = lax.switch(
        role,
        [
            lambda month, mix: reader(month),
            lambda month, mix: reader(mix),
            lambda month, mix: pl.pallas_call(blank, out_shape=row, out_specs=vmem)(),
        ],
        month,
        mix,
    )
    share = pl.pallas_call(
        functools.partial(kernel, n, m),
        out_shape=pltpu.VMEM((types, cells), f32),
        in_specs=[vmem] + [hbm] * 6,
        out_specs=vmem,
        scratch_shapes=[
            pltpu.VMEM(soil_water.shape, f32),
            pltpu.VMEM(root_share.shape, f32),
            pltpu.VMEM(patch_weight.shape, f32),
            pltpu.VMEM(owner.shape, i32),
            pltpu.VMEM(local.shape, i32),
            pltpu.VMEM((m, months, types, cells), f32),
            pltpu.VMEM((2, *row.shape), f32),
            pltpu.VMEM((n, types, cells), f32),
            pltpu.VMEM((m, 2, types, cells), f32),
            pltpu.VMEM((n, m, types, cells), f32),
            pltpu.VMEM((rows, cells), f32),
            *[pltpu.SemaphoreType.DMA] * 2,
            pltpu.SemaphoreType.REGULAR,
        ],
        compiler_params=pltpu.CompilerParams(collective_id=0, has_side_effects=True),
    )(given, leaf_area, soil_water, root_share, patch_weight, owner, local)
    return pl.pallas_call(
        put_rows,
        out_shape=jax.ShapeDtypeStruct(share.shape, f32),
        in_specs=[vmem],
        out_specs=hbm,
    )(pltpu.with_memory_space_constraint(share, pltpu.VMEM))


def solution(mesh):
    in_specs = (
        P(None, "layer", "blk"),
        P(None, "blk"),
        P("layer", None),
        P("layer", "blk"),
        P("blk", None),
        P("blk"),
        P(),
        P(),
    )
    out_specs = P("layer", "blk")
    return jax.shard_map(
        on_device, mesh=mesh, in_specs=in_specs, out_specs=out_specs, check_vma=False
    )
```
